128 devices in a mesh: rad: 32 (over y, z, core), ang: 4 (over x).
Axes of the slice: x: 4, y: 4, z: 4, core: 2. Of those that a mesh axis runs over, the one named last changes fastest.
Arguments:
- nonlin: bfloat16 [2, 512, 131072], P(None, 'rad', 'ang'), may hold values from -6 to 6
- state: float32 [2, 512, 131072], P(None, 'rad', 'ang'), may hold values from -6 to 6
- inverse: float32 [128, 2, 1024, 1024], P(('ang', 'rad')), may hold values from -0.1875 to 0.1875
- pair_of_slot: int32 [128], P(('ang', 'rad')), may hold values from 0 to 127, each once
Outputs:
- new_state: float32 [2, 512, 131072], P(None, 'rad', 'ang')
The draws below stay inside these ranges and needn't reach their ends.
Inputs may be any that keep to these rules, and one draw needn't show every extreme that they name: Slot s of the window holds degrees pair_of_slot[s] and 511 - pair_of_slot[s]; every pair once.
All inputs are finite; a program needn't handle non-finite values.
Results may differ from the reference program's by a relative error of at most 0.0003.
Values may be sent and summed in bfloat16 or wider, within the bound.
A program may use at most 128 MiB of HBM per device.

```python
import math
import jax
import jax.numpy as jnp
from jax import lax

LMAX = 511
NR = 512
NPAIR = 128
NCOL = 131072


def levels(own_key, shape, split, smallest, top_value):
    def one(position, parts):
        draws = jax.random.uniform(jax.random.fold_in(jax.random.fold_in(own_key, 6), position), (parts,), jnp.float32, smallest / len(split), top_value / len(split))
        return jnp.repeat(jnp.exp(draws), shape[position] // parts).reshape((-1,) + (1,) * (len(shape) - position - 1))

    factor_of = one(*split[0])
    for cut in split[1:]:
        factor_of = factor_of * one(*cut)
    return factor_of


def bell_draw(rng, shape, width, bound, pieces=(), kind=jnp.bfloat16):
    loudness = levels(rng, shape, pieces, -0.22, 0.18) if pieces else 1.0
    result = jax.random.normal(rng, shape, jnp.float32) * width * loudness
    return jnp.minimum(jnp.maximum(result, -bound), bound).astype(kind)


def setup_inputs(seed: int = 0) -> dict:
    splits = jax.random.split(jax.random.key(seed), 5)
    nonlin = bell_draw(splits[0], (2, NR, NCOL), 1.0, 6.0, ((1, 32), (2, 4)))
    state = bell_draw(splits[1], (2, NR, NCOL), 1.0, 6.0, ((1, 32), (2, 4)), jnp.float32)
    inverse = bell_draw(splits[2], (NPAIR, 2, 2 * NR, 2 * NR), (2 * NR) ** -0.5, 0.1875, ((0, 128),), jnp.float32)
    pair_of_slot = jax.random.permutation(splits[3], NPAIR).astype(jnp.int32)
    return {"nonlin": nonlin, "state": state, "inverse": inverse, "pair_of_slot": pair_of_slot}


inner_radius = 0.35
outer_radius = 1.0
blend_weight = 0.5


def radius_at(level_index, total_levels):
    scaled = level_index / (total_levels - 1.0)
    stretch = (1.0 - blend_weight) * scaled + blend_weight * (1.0 - jnp.cos(math.pi * scaled)) / 2.0
    return inner_radius + (outer_radius - inner_radius) * stretch


def forcing(padded, old_state, first_level, total_levels):
    count = padded.shape[1] - 2
    values = padded.astype(jnp.float32)
    level_index = jnp.arange(count, dtype=jnp.float32) + first_level
    radius_here = radius_at(level_index, total_levels)
    step_below = radius_here - radius_at(level_index - 1.0, total_levels)
    step_above = radius_at(level_index + 1.0, total_levels) - radius_here
    at_inner = level_index == 0.0
    at_outer = level_index == total_levels - 1.0
    weight_below = jnp.where(at_inner, 0.0, jnp.where(at_outer, -1.0 / step_below, -step_above / (step_below * (step_below + step_above))))
    weight_here = jnp.where(at_inner, -1.0 / step_above, jnp.where(at_outer, 1.0 / step_below, (step_above - step_below) / (step_below * step_above)))
    weight_above = jnp.where(at_inner, 1.0 / step_above, jnp.where(at_outer, 0.0, step_below / (step_above * (step_below + step_above))))
    centre = values[:, 1:-1]
    derivative = weight_below[None, :, None] * values[:, :-2] + weight_here[None, :, None] * centre + weight_above[None, :, None] * values[:, 2:]
    time_step = 0.5 * (outer_radius - inner_radius) / (total_levels - 1.0)
    return old_state + time_step * (derivative + 2.0 * centre / radius_here[None, :, None])


def lower_mask(column_count, pair_index):
    half_cols = column_count // 2
    column_index = jnp.arange(column_count, dtype=jnp.int32)
    first_half = column_index < pair_index + 1
    second_half = (column_index >= half_cols) & (column_index - half_cols < pair_index)
    return jnp.where(column_index < half_cols, first_half, second_half)


def apply_inverse(block, matrices, pair_index):
    field_count, level_count, column_count = block.shape
    flattened = block.reshape(field_count * level_count, column_count)
    lower_part = jnp.dot(matrices[0], flattened, precision=lax.Precision.HIGHEST, preferred_element_type=jnp.float32)
    upper_part = jnp.dot(matrices[1], flattened, precision=lax.Precision.HIGHEST, preferred_element_type=jnp.float32)
    chosen = jnp.where(lower_mask(column_count, pair_index)[None, :], lower_part, upper_part)
    return chosen.reshape(field_count, level_count, column_count)


def reference(nonlin, state, inverse, pair_of_slot):
    level_count = nonlin.shape[1]
    padded = jnp.pad(nonlin, ((0, 0), (1, 1), (0, 0)))
    right_side = forcing(padded, state, jnp.float32(0.0), level_count * 1.0)
    column_count = 2 * (LMAX + 1)
    slot_count = right_side.shape[2] // column_count
    blocks = right_side.reshape(2, level_count, slot_count, column_count).transpose(2, 0, 1, 3)

    def one_slot(packed):
        block, matrices, pair_index = packed
        return apply_inverse(block, matrices, pair_index)

    solved = lax.map(one_slot, (blocks, inverse, pair_of_slot))
    return solved.transpose(1, 2, 0, 3).reshape(2, level_count, slot_count * column_count)
```

```python
import functools
import math

import jax
import jax.numpy as jnp
import numpy as np
from jax import lax
from jax.experimental import pallas as pl
from jax.experimental.pallas import tpu as pltpu
from jax.sharding import PartitionSpec as P

inner_radius = 0.35
outer_radius = 1.0
blend_weight = 0.5

MESH = pl.DeviceIdType.MESH
LANES = 128
CHUNK_TILES = ((0, 4), (1, 2), (3, 5), (6, 7))
MIXED = 0
QMAX = 32767.0
TINY = 1e-30


def level_weights(total_levels):
    def radius_at(k):
        scaled = k / (total_levels - 1.0)
        stretch = (1.0 - blend_weight) * scaled + blend_weight * (1.0 - np.cos(math.pi * scaled)) / 2.0
        return inner_radius + (outer_radius - inner_radius) * stretch

    k = np.arange(total_levels, dtype=np.float64)
    here = radius_at(k)
    below = here - radius_at(k - 1.0)
    above = radius_at(k + 1.0) - here
    weight_below = -above / (below * (below + above))
    weight_here = (above - below) / (below * above)
    weight_above = below / (above * (below + above))
    weight_below[0], weight_here[0], weight_above[0] = 0.0, -1.0 / above[0], 1.0 / above[0]
    weight_below[-1], weight_here[-1], weight_above[-1] = -1.0 / below[-1], 1.0 / below[-1], 0.0
    dt = 0.5 * (outer_radius - inner_radius) / (total_levels - 1.0)
    return np.stack([dt * weight_below, dt * (weight_here + 2.0 / here), dt * weight_above], 0)


def step_kernel(
    groups, levels, width,
    weights_ref, nonlin_ref, state_ref, inverse_ref, pair_ref,
    outq_ref, outs_ref,
    nl, st, wt, minv, mhi, mlo, halo_f, halo_out, halo_in,
    fsrc, fdst, fss, fsd, vhi, vlo, y, bsrc, bss, outs_v,
    load_sem, inv_sem, halo_ssem, halo_rsem,
    fsend, frecv, fs_send, fs_recv, bsend, brecv, bs_send, bs_recv, out_sem,
):
    chunks = len(CHUNK_TILES)
    me = lax.axis_index("rad")
    half = groups * levels
    cw = width // chunks

    barrier = pltpu.get_barrier_semaphore()

    @pl.loop(1, groups)
    def _(j):
        pl.semaphore_signal(barrier, inc=1, device_id={"rad": lax.rem(me + j, groups)}, device_id_type=MESH)

    load_nl = pltpu.make_async_copy(nonlin_ref, nl, load_sem.at[0])
    load_st = pltpu.make_async_copy(state_ref, st, load_sem.at[1])
    load_wt = pltpu.make_async_copy(weights_ref.at[me], wt, load_sem.at[2])
    load_nl.start()
    load_wt.start()
    load_st.start()
    load_inv = [pltpu.make_async_copy(inverse_ref.at[0, m], minv.at[m], inv_sem.at[m]) for m in range(2)]
    for copy in load_inv:
        copy.start()

    load_nl.wait()

    @pl.loop(0, groups)
    def _(s):
        for f in range(2):
            for t in range(width // LANES):
                cols = pl.ds(pl.multiple_of(s * width + t * LANES, LANES), LANES)
                rows = nl[f, :, cols].astype(jnp.float32)
                at = f * (width // LANES) + t
                halo_f[0, s, at:at + 1, :] = rows[levels - 1:levels]
                halo_f[1, s, at:at + 1, :] = rows[0:1]
        for d in range(2):
            halo_out[d, s] = halo_f[d, s].astype(jnp.bfloat16)

    pl.semaphore_wait(barrier, groups - 1)
    halo_copies = []
    for d, peer in ((0, lax.rem(me + 1, groups)), (1, lax.rem(me + groups - 1, groups))):
        halo_copies.append(pltpu.make_async_remote_copy(
            src_ref=halo_out.at[d], dst_ref=halo_in.at[d], send_sem=halo_ssem.at[d], recv_sem=halo_rsem.at[d],
            device_id={"rad": peer}, device_id_type=MESH))
    for copy in halo_copies:
        copy.start()

    for m in range(2):
        load_inv[m].wait()

        @pl.loop(0, 2 * half // 64)
        def _(i, m=m):
            rows = pl.ds(pl.multiple_of(i * 64, 64), 64)
            full = minv[m, rows, :]
            high = full.astype(jnp.bfloat16)
            mhi[m, rows, :] = high
            mlo[m, rows, :] = (full - high.astype(jnp.float32)).astype(jnp.bfloat16)

    load_st.wait()
    load_wt.wait()
    for copy in halo_copies:
        copy.wait()

    def forward_copy(ch, peer):
        return pltpu.make_async_remote_copy(
            src_ref=fsrc.at[ch, peer], dst_ref=fdst.at[ch, :, me], send_sem=fsend.at[ch], recv_sem=frecv.at[ch],
            device_id={"rad": peer}, device_id_type=MESH)

    def forward_own(ch):
        return pltpu.make_async_copy(fsrc.at[ch, me], fdst.at[ch, :, me], frecv.at[ch])

    row_index = lax.broadcasted_iota(jnp.int32, (levels, LANES), 0)

    @pl.loop(0, groups)
    def _(j):
        peer = lax.rem(me + j, groups)
        col0 = pl.multiple_of(peer * width, width)
        edges = [halo_in[d, peer].astype(jnp.float32) for d in range(2)]
        tiles = {}
        largest = None
        for f in range(2):
            for t in range(width // LANES):
                cols = pl.ds(pl.multiple_of(col0 + t * LANES, LANES), LANES)
                here = nl[f, :, cols].astype(jnp.float32)
                at = f * (width // LANES) + t
                low, top = edges[0][at:at + 1], edges[1][at:at + 1]
                below = jnp.where(row_index == 0, low, pltpu.roll(here, 1, 0))
                above = jnp.where(row_index == levels - 1, top, pltpu.roll(here, levels - 1, 0))
                value = st[f, :, cols] + (wt[0] * below + wt[1] * here + wt[2] * above)
                tiles[f, t] = value
                size = jnp.abs(value)
                largest = size if largest is None else jnp.maximum(largest, size)
        largest = jnp.maximum(jnp.max(largest, axis=0, keepdims=True), TINY)
        fss[peer] = largest * (1.0 / QMAX)
        factor = QMAX / largest
        for ch, members in enumerate(CHUNK_TILES):
            for n, t in enumerate(members):
                for f in range(2):
                    code = jnp.round(tiles[f, t] * factor).astype(jnp.int32).astype(jnp.int16)
                    fsrc[ch, peer, f, :, n * LANES:(n + 1) * LANES] = code

        @pl.when(j > 0)
        def _():
            pltpu.make_async_remote_copy(
                src_ref=fss.at[peer], dst_ref=fsd.at[me], send_sem=fs_send, recv_sem=fs_recv,
                device_id={"rad": peer}, device_id_type=MESH).start()
            forward_copy(0, peer).start()

        @pl.when(j == 0)
        def _():
            pltpu.make_async_copy(fss.at[me], fsd.at[me], fs_recv).start()
            forward_own(0).start()

    for ch in range(1, chunks):
        forward_own(ch).start()

        @pl.loop(1, groups)
        def _(j, ch=ch):
            forward_copy(ch, lax.rem(me + j, groups)).start()

    pair = pair_ref[0]
    pltpu.make_async_copy(fsd, fsd, fs_recv).wait()
    for ch, members in enumerate(CHUNK_TILES):
        pltpu.make_async_copy(fdst.at[ch], fdst.at[ch], frecv.at[ch]).wait()

        @pl.loop(0, groups)
        def _(r, ch=ch):
            scale = jnp.concatenate([fsd[r]] * (cw // LANES), axis=1)
            for f in range(2):
                value = fdst[ch, f, r].astype(jnp.int32).astype(jnp.float32) * scale
                high = value.astype(jnp.bfloat16)
                rows = pl.ds(pl.multiple_of(f * half + r * levels, levels), levels)
                vhi[rows, :] = high
                vlo[rows, :] = (value - high.astype(jnp.float32)).astype(jnp.bfloat16)

        @pl.loop(0, 2 * half // 256)
        def _(i, ch=ch, members=members):
            rows = pl.ds(pl.multiple_of(i * 256, 256), 256)

            def product(m):
                dot = functools.partial(jnp.dot, preferred_element_type=jnp.float32)
                return (dot(mhi[m, rows, :], vhi[...]) + dot(mhi[m, rows, :], vlo[...])) + dot(mlo[m, rows, :], vhi[...])

            upper = product(1)
            if ch == MIXED:
                lower = product(0)
                lane = lax.broadcasted_iota(jnp.int32, (256, cw), 1)
                order = jnp.where(lane < LANES, lane, lane - LANES + 1)
                y[rows, :] = jnp.where(order < pair + 1, lower, upper)
            else:
                y[rows, :] = upper

        @pl.loop(0, groups)
        def _(j, ch=ch):
            peer = lax.rem(me + j, groups)
            values = [
                y[pl.ds(pl.multiple_of(f * half + peer * levels, levels), levels), n * LANES:(n + 1) * LANES]
                for f in range(2) for n in range(cw // LANES)
            ]
            largest = functools.reduce(jnp.maximum, [jnp.abs(value) for value in values])
            largest = jnp.maximum(jnp.max(largest, axis=0, keepdims=True), TINY)
            bss[ch, peer] = largest * (1.0 / QMAX)
            factor = QMAX / largest
            for f in range(2):
                for n in range(cw // LANES):
                    value = values[f * (cw // LANES) + n]
                    code = jnp.round(value * factor).astype(jnp.int32).astype(jnp.int16)
                    bsrc[ch, peer, f, :, n * LANES:(n + 1) * LANES] = code

            @pl.when(j > 0)
            def _():
                pltpu.make_async_remote_copy(
                    src_ref=bss.at[ch, peer], dst_ref=outs_v.at[ch, me], send_sem=bs_send.at[ch],
                    recv_sem=bs_recv.at[ch], device_id={"rad": peer}, device_id_type=MESH).start()
                pltpu.make_async_remote_copy(
                    src_ref=bsrc.at[ch, peer], dst_ref=outq_ref.at[ch, me], send_sem=bsend.at[ch],
                    recv_sem=brecv.at[ch], device_id={"rad": peer}, device_id_type=MESH).start()

            @pl.when(j == 0)
            def _():
                pltpu.make_async_copy(bss.at[ch, me], outs_v.at[ch, me], bs_recv.at[ch]).start()
                pltpu.make_async_copy(bsrc.at[ch, me], outq_ref.at[ch, me], brecv.at[ch]).start()

    others = pl.ds(0, groups - 1)
    for ch in range(chunks):
        pltpu.make_async_copy(outs_v.at[ch], outs_v.at[ch], bs_recv.at[ch]).wait()
    store = pltpu.make_async_copy(outs_v, outs_ref, out_sem)
    store.start()
    pltpu.make_async_copy(fss.at[others], fss.at[others], fs_send).wait()
    for ch in range(chunks):
        pltpu.make_async_copy(fsrc.at[ch, others], fsrc.at[ch, others], fsend.at[ch]).wait()
        pltpu.make_async_copy(bsrc.at[ch, others], bsrc.at[ch, others], bsend.at[ch]).wait()
        pltpu.make_async_copy(bss.at[ch, others], bss.at[ch, others], bs_send.at[ch]).wait()
        pltpu.make_async_copy(outq_ref.at[ch], outq_ref.at[ch], brecv.at[ch]).wait()
    store.wait()


def decode_kernel(slots, width, q_ref, s_ref, o_ref):
    for s in range(slots):
        for ch, members in enumerate(CHUNK_TILES):
            scale = s_ref[ch, s]
            for n, t in enumerate(members):
                for f in range(2):
                    code = q_ref[ch, s, f, :, n * LANES:(n + 1) * LANES]
                    o_ref[f, :, s * width + t * LANES:s * width + (t + 1) * LANES] = (
                        code.astype(jnp.int32).astype(jnp.float32) * scale
                    )


def local(nonlin, state, inverse, pair_of_slot):
    levels = nonlin.shape[1]
    groups = lax.axis_size("rad")
    width = nonlin.shape[2] // groups
    total = levels * groups
    chunks = len(CHUNK_TILES)
    cw = width // chunks
    weights = level_weights(total).reshape(3, groups, levels).transpose(1, 0, 2)[..., None]
    weights = jnp.asarray(np.broadcast_to(weights, (groups, 3, levels, LANES)).astype(np.float32))
    anywhere = pl.BlockSpec(memory_space=pl.ANY)
    q_shape = (chunks, groups, 2, levels, cw)
    s_shape = (chunks, groups, 1, LANES)
    dma = pltpu.SemaphoreType.DMA
    outq, outs = pl.pallas_call(
        functools.partial(step_kernel, groups, levels, width),
        out_shape=(jax.ShapeDtypeStruct(q_shape, jnp.int16), jax.ShapeDtypeStruct(s_shape, jnp.float32)),
        in_specs=[anywhere] * 4 + [pl.BlockSpec(memory_space=pltpu.SMEM)],
        out_specs=(anywhere, anywhere),
        scratch_shapes=[
            pltpu.VMEM(nonlin.shape, jnp.bfloat16),
            pltpu.VMEM(state.shape, jnp.float32),
            pltpu.VMEM((3, levels, LANES), jnp.float32),
            pltpu.VMEM((2, 2 * total, 2 * total), jnp.float32),
            pltpu.VMEM((2, 2 * total, 2 * total), jnp.bfloat16),
            pltpu.VMEM((2, 2 * total, 2 * total), jnp.bfloat16),
            pltpu.VMEM((2, groups, 2 * width // LANES, LANES), jnp.float32),
            pltpu.VMEM((2, groups, 2 * width // LANES, LANES), jnp.bfloat16),
            pltpu.VMEM((2, groups, 2 * width // LANES, LANES), jnp.bfloat16),
            pltpu.VMEM(q_shape, jnp.int16),
            pltpu.VMEM((chunks, 2, groups, levels, cw), jnp.int16),
            pltpu.VMEM((groups, 1, LANES), jnp.float32),
            pltpu.VMEM((groups, 1, LANES), jnp.float32),
            pltpu.VMEM((2 * total, cw), jnp.bfloat16),
            pltpu.VMEM((2 * total, cw), jnp.bfloat16),
            pltpu.VMEM((2 * total, cw), jnp.float32),
            pltpu.VMEM(q_shape, jnp.int16),
            pltpu.VMEM(s_shape, jnp.float32),
            pltpu.VMEM(s_shape, jnp.float32),
            dma((3,)), dma((2,)), dma((2,)), dma((2,)),
            dma((chunks,)), dma((chunks,)), dma, dma,
            dma((chunks,)), dma((chunks,)), dma((chunks,)), dma((chunks,)), dma,
        ],
        compiler_params=pltpu.CompilerParams(
            collective_id=0, has_side_effects=True, vmem_limit_bytes=56 * 2**20),
        name="radial_step",
    )(weights, nonlin, state, inverse, pair_of_slot)

    slots = 4
    return pl.pallas_call(
        functools.partial(decode_kernel, slots, width),
        out_shape=jax.ShapeDtypeStruct(state.shape, jnp.float32),
        grid=(groups // slots,),
        in_specs=[
            pl.BlockSpec((chunks, slots, 2, levels, cw), lambda i: (0, i, 0, 0, 0)),
            pl.BlockSpec((chunks, slots, 1, LANES), lambda i: (0, i, 0, 0)),
        ],
        out_specs=pl.BlockSpec((2, levels, slots * width), lambda i: (0, 0, i)),
        name="decode",
    )(outq, outs)


def solution(mesh):
    placed = (
        P(None, "rad", "ang"),
        P(None, "rad", "ang"),
        P(("ang", "rad"), None, None, None),
        P(("ang", "rad")),
    )
    return jax.shard_map(
        local, mesh=mesh, in_specs=placed, out_specs=P(None, "rad", "ang"), check_vma=False
    )
```

```python
import functools
import math

import jax
import jax.numpy as jnp
import numpy as np
from jax import lax
from jax.experimental import pallas as pl
from jax.experimental.pallas import tpu as pltpu
from jax.sharding import PartitionSpec as P

inner_radius = 0.35
outer_radius = 1.0
blend_weight = 0.5

MESH = pl.DeviceIdType.MESH
LANES = 128
CHUNK_TILES = ((0, 4), (1, 2), (3, 5), (6, 7))
MIXED = 0
QMAX = 32767.0
TINY = 1e-30
ORDER = (
    8, 24, 2, 20, 6, 12, 28, 10, 30, 4, 16, 14, 26, 18, 22, 9,
    25, 3, 21, 7, 13, 29, 11, 31, 5, 17, 15, 27, 19, 23, 1,
)


def offset_words(order):
    padded = [0] + list(order)
    return [sum(d << (5 * n) for n, d in enumerate(padded[i:i + 4])) for i in range(0, len(padded), 4)]


def peer_at(me, j):
    word = functools.reduce(
        lambda rest, n: jnp.where(j // 4 == n, WORDS[n], rest), range(1, len(WORDS)), WORDS[0])
    step = (word >> (5 * lax.rem(j, 4))) & 31
    return ((me + (step & 24)) & 24) | ((me + (step & 6)) & 6) | ((me ^ step) & 1)


WORDS = offset_words(ORDER)


def level_weights(total_levels):
    def radius_at(k):
        scaled = k / (total_levels - 1.0)
        stretch = (1.0 - blend_weight) * scaled + blend_weight * (1.0 - np.cos(math.pi * scaled)) / 2.0
        return inner_radius + (outer_radius - inner_radius) * stretch

    k = np.arange(total_levels, dtype=np.float64)
    here = radius_at(k)
    below = here - radius_at(k - 1.0)
    above = radius_at(k + 1.0) - here
    weight_below = -above / (below * (below + above))
    weight_here = (above - below) / (below * above)
    weight_above = below / (above * (below + above))
    weight_below[0], weight_here[0], weight_above[0] = 0.0, -1.0 / above[0], 1.0 / above[0]
    weight_below[-1], weight_here[-1], weight_above[-1] = -1.0 / below[-1], 1.0 / below[-1], 0.0
    dt = 0.5 * (outer_radius - inner_radius) / (total_levels - 1.0)
    return np.stack([dt * weight_below, dt * (weight_here + 2.0 / here), dt * weight_above], 0)


def step_kernel(
    groups, levels, width,
    weights_ref, nonlin_ref, state_ref, inverse_ref, pair_ref,
    outq_ref, outs_ref,
    nl, st, wt, minv, mhi, mlo, halo_f, halo_out, halo_in,
    fsrc, fdst, fss, fsd, vhi, vlo, y, bsrc, bss, outs_v,
    load_sem, inv_sem, halo_ssem, halo_rsem,
    fsend, frecv, fs_send, fs_recv, bsend, brecv, bs_send, bs_recv, out_sem,
):
    chunks = len(CHUNK_TILES)
    me = lax.axis_index("rad")
    half = groups * levels
    cw = width // chunks

    barrier = pltpu.get_barrier_semaphore()

    @pl.loop(1, groups)
    def _(j):
        pl.semaphore_signal(barrier, inc=1, device_id={"rad": lax.rem(me + j, groups)}, device_id_type=MESH)

    load_nl = pltpu.make_async_copy(nonlin_ref, nl, load_sem.at[0])
    load_st = pltpu.make_async_copy(state_ref, st, load_sem.at[1])
    load_wt = pltpu.make_async_copy(weights_ref.at[me], wt, load_sem.at[2])
    load_nl.start()
    load_wt.start()
    load_st.start()
    load_inv = [pltpu.make_async_copy(inverse_ref.at[0, m], minv.at[m], inv_sem.at[m]) for m in range(2)]
    for copy in load_inv:
        copy.start()

    load_nl.wait()

    @pl.loop(0, groups)
    def _(s):
        for f in range(2):
            for t in range(width // LANES):
                cols = pl.ds(pl.multiple_of(s * width + t * LANES, LANES), LANES)
                rows = nl[f, :, cols].astype(jnp.float32)
                at = f * (width // LANES) + t
                halo_f[0, s, at:at + 1, :] = rows[levels - 1:levels]
                halo_f[1, s, at:at + 1, :] = rows[0:1]
        for d in range(2):
            halo_out[d, s] = halo_f[d, s].astype(jnp.bfloat16)

    pl.semaphore_wait(barrier, groups - 1)
    halo_copies = []
    for d, peer in ((0, lax.rem(me + 1, groups)), (1, lax.rem(me + groups - 1, groups))):
        halo_copies.append(pltpu.make_async_remote_copy(
            src_ref=halo_out.at[d], dst_ref=halo_in.at[d], send_sem=halo_ssem.at[d], recv_sem=halo_rsem.at[d],
            device_id={"rad": peer}, device_id_type=MESH))
    for copy in halo_copies:
        copy.start()

    load_st.wait()
    load_wt.wait()
    for copy in halo_copies:
        copy.wait()

    def forward_copy(ch, peer):
        return pltpu.make_async_remote_copy(
            src_ref=fsrc.at[ch, peer], dst_ref=fdst.at[ch, :, me], send_sem=fsend.at[ch], recv_sem=frecv.at[ch],
            device_id={"rad": peer}, device_id_type=MESH)

    def forward_own(ch):
        return pltpu.make_async_copy(fsrc.at[ch, me], fdst.at[ch, :, me], frecv.at[ch])

    row_index = lax.broadcasted_iota(jnp.int32, (levels, LANES), 0)

    @pl.loop(0, groups)
    def _(j):
        peer = peer_at(me, j)
        col0 = pl.multiple_of(peer * width, width)
        edges = [halo_in[d, peer].astype(jnp.float32) for d in range(2)]
        tiles = {}
        largest = None
        for f in range(2):
            for t in range(width // LANES):
                cols = pl.ds(pl.multiple_of(col0 + t * LANES, LANES), LANES)
                here = nl[f, :, cols].astype(jnp.float32)
                at = f * (width // LANES) + t
                low, top = edges[0][at:at + 1], edges[1][at:at + 1]
                below = jnp.where(row_index == 0, low, pltpu.roll(here, 1, 0))
                above = jnp.where(row_index == levels - 1, top, pltpu.roll(here, levels - 1, 0))
                value = st[f, :, cols] + (wt[0] * below + wt[1] * here + wt[2] * above)
                tiles[f, t] = value
                size = jnp.abs(value)
                largest = size if largest is None else jnp.maximum(largest, size)
        largest = jnp.maximum(jnp.max(largest, axis=0, keepdims=True), TINY)
        fss[peer] = largest * (1.0 / QMAX)
        factor = QMAX / largest
        for ch, members in enumerate(CHUNK_TILES):
            for n, t in enumerate(members):
                for f in range(2):
                    code = jnp.round(tiles[f, t] * factor).astype(jnp.int32).astype(jnp.int16)
                    fsrc[ch, peer, f, :, n * LANES:(n + 1) * LANES] = code

        @pl.when(j > 0)
        def _():
            pltpu.make_async_remote_copy(
                src_ref=fss.at[peer], dst_ref=fsd.at[me], send_sem=fs_send, recv_sem=fs_recv,
                device_id={"rad": peer}, device_id_type=MESH).start()
            forward_copy(0, peer).start()

        @pl.when(j == 0)
        def _():
            pltpu.make_async_copy(fss.at[me], fsd.at[me], fs_recv).start()
            forward_own(0).start()

    for ch in range(1, chunks):
        forward_own(ch).start()

        @pl.loop(1, groups)
        def _(j, ch=ch):
            forward_copy(ch, peer_at(me, j)).start()

    for m in range(2):
        load_inv[m].wait()

        @pl.loop(0, 2 * half // 64)
        def _(i, m=m):
            rows = pl.ds(pl.multiple_of(i * 64, 64), 64)
            full = minv[m, rows, :]
            high = full.astype(jnp.bfloat16)
            mhi[m, rows, :] = high
            mlo[m, rows, :] = (full - high.astype(jnp.float32)).astype(jnp.bfloat16)

    pair = pair_ref[0]
    pltpu.make_async_copy(fsd, fsd, fs_recv).wait()
    for ch, members in enumerate(CHUNK_TILES):
        pltpu.make_async_copy(fdst.at[ch], fdst.at[ch], frecv.at[ch]).wait()

        @pl.loop(0, groups)
        def _(r, ch=ch):
            scale = jnp.concatenate([fsd[r]] * (cw // LANES), axis=1)
            for f in range(2):
                value = fdst[ch, f, r].astype(jnp.int32).astype(jnp.float32) * scale
                high = value.astype(jnp.bfloat16)
                rows = pl.ds(pl.multiple_of(f * half + r * levels, levels), levels)
                vhi[rows, :] = high
                vlo[rows, :] = (value - high.astype(jnp.float32)).astype(jnp.bfloat16)

        @pl.loop(0, 2 * half // 256)
        def _(i, ch=ch, members=members):
            rows = pl.ds(pl.multiple_of(i * 256, 256), 256)

            def product(m):
                dot = functools.partial(jnp.dot, preferred_element_type=jnp.float32)
                return (dot(mhi[m, rows, :], vhi[...]) + dot(mhi[m, rows, :], vlo[...])) + dot(mlo[m, rows, :], vhi[...])

            upper = product(1)
            if ch == MIXED:
                lower = product(0)
                lane = lax.broadcasted_iota(jnp.int32, (256, cw), 1)
                order = jnp.where(lane < LANES, lane, lane - LANES + 1)
                y[rows, :] = jnp.where(order < pair + 1, lower, upper)
            else:
                y[rows, :] = upper

        @pl.loop(0, groups)
        def _(j, ch=ch):
            peer = peer_at(me, j)
            values = [
                y[pl.ds(pl.multiple_of(f * half + peer * levels, levels), levels), n * LANES:(n + 1) * LANES]
                for f in range(2) for n in range(cw // LANES)
            ]
            largest = functools.reduce(jnp.maximum, [jnp.abs(value) for value in values])
            largest = jnp.maximum(jnp.max(largest, axis=0, keepdims=True), TINY)
            bss[ch, peer] = largest * (1.0 / QMAX)
            factor = QMAX / largest
            for f in range(2):
                for n in range(cw // LANES):
                    value = values[f * (cw // LANES) + n]
                    code = jnp.round(value * factor).astype(jnp.int32).astype(jnp.int16)
                    bsrc[ch, peer, f, :, n * LANES:(n + 1) * LANES] = code

            @pl.when(j > 0)
            def _():
                pltpu.make_async_remote_copy(
                    src_ref=bss.at[ch, peer], dst_ref=outs_v.at[ch, me], send_sem=bs_send.at[ch],
                    recv_sem=bs_recv.at[ch], device_id={"rad": peer}, device_id_type=MESH).start()
                pltpu.make_async_remote_copy(
                    src_ref=bsrc.at[ch, peer], dst_ref=outq_ref.at[ch, me], send_sem=bsend.at[ch],
                    recv_sem=brecv.at[ch], device_id={"rad": peer}, device_id_type=MESH).start()

            @pl.when(j == 0)
            def _():
                pltpu.make_async_copy(bss.at[ch, me], outs_v.at[ch, me], bs_recv.at[ch]).start()
                pltpu.make_async_copy(bsrc.at[ch, me], outq_ref.at[ch, me], brecv.at[ch]).start()

    others = pl.ds(0, groups - 1)
    for ch in range(chunks):
        pltpu.make_async_copy(outs_v.at[ch], outs_v.at[ch], bs_recv.at[ch]).wait()
    store = pltpu.make_async_copy(outs_v, outs_ref, out_sem)
    store.start()
    pltpu.make_async_copy(fss.at[others], fss.at[others], fs_send).wait()
    for ch in range(chunks):
        pltpu.make_async_copy(fsrc.at[ch, others], fsrc.at[ch, others], fsend.at[ch]).wait()
        pltpu.make_async_copy(bsrc.at[ch, others], bsrc.at[ch, others], bsend.at[ch]).wait()
        pltpu.make_async_copy(bss.at[ch, others], bss.at[ch, others], bs_send.at[ch]).wait()
        pltpu.make_async_copy(outq_ref.at[ch], outq_ref.at[ch], brecv.at[ch]).wait()
    store.wait()


def decode_kernel(parts, groups, width, q_ref, s_ref, o_ref, q, s, o, s_sem, in_sem, out_sem):
    each = groups // parts
    scales = pltpu.make_async_copy(s_ref, s, s_sem)
    scales.start()

    def load(i):
        slots = pl.ds(i * each, each)
        return pltpu.make_async_copy(q_ref.at[:, slots], q.at[:, slots], in_sem.at[i])

    def store(i):
        cols = pl.ds(pl.multiple_of(i * each * width, each * width), each * width)
        return pltpu.make_async_copy(o.at[:, :, cols], o_ref.at[:, :, cols], out_sem.at[i])

    for i in range(parts):
        load(i).start()
    scales.wait()

    @pl.loop(0, parts)
    def _(i):
        load(i).wait()
        for k in range(each):
            slot = i * each + k
            for ch, members in enumerate(CHUNK_TILES):
                scale = s[ch, slot]
                for n, t in enumerate(members):
                    cols = pl.ds(pl.multiple_of(slot * width + t * LANES, LANES), LANES)
                    for f in range(2):
                        code = q[ch, slot, f, :, n * LANES:(n + 1) * LANES]
                        o[f, :, cols] = code.astype(jnp.int32).astype(jnp.float32) * scale
        store(i).start()

    for i in range(parts):
        store(i).wait()


def local(nonlin, state, inverse, pair_of_slot):
    levels = nonlin.shape[1]
    groups = lax.axis_size("rad")
    width = nonlin.shape[2] // groups
    total = levels * groups
    chunks = len(CHUNK_TILES)
    cw = width // chunks
    weights = level_weights(total).reshape(3, groups, levels).transpose(1, 0, 2)[..., None]
    weights = jnp.asarray(np.broadcast_to(weights, (groups, 3, levels, LANES)).astype(np.float32))
    anywhere = pl.BlockSpec(memory_space=pl.ANY)
    q_shape = (chunks, groups, 2, levels, cw)
    s_shape = (chunks, groups, 1, LANES)
    dma = pltpu.SemaphoreType.DMA
    outq, outs = pl.pallas_call(
        functools.partial(step_kernel, groups, levels, width),
        out_shape=(jax.ShapeDtypeStruct(q_shape, jnp.int16), jax.ShapeDtypeStruct(s_shape, jnp.float32)),
        in_specs=[anywhere] * 4 + [pl.BlockSpec(memory_space=pltpu.SMEM)],
        out_specs=(anywhere, anywhere),
        scratch_shapes=[
            pltpu.VMEM(nonlin.shape, jnp.bfloat16),
            pltpu.VMEM(state.shape, jnp.float32),
            pltpu.VMEM((3, levels, LANES), jnp.float32),
            pltpu.VMEM((2, 2 * total, 2 * total), jnp.float32),
            pltpu.VMEM((2, 2 * total, 2 * total), jnp.bfloat16),
            pltpu.VMEM((2, 2 * total, 2 * total), jnp.bfloat16),
            pltpu.VMEM((2, groups, 2 * width // LANES, LANES), jnp.float32),
            pltpu.VMEM((2, groups, 2 * width // LANES, LANES), jnp.bfloat16),
            pltpu.VMEM((2, groups, 2 * width // LANES, LANES), jnp.bfloat16),
            pltpu.VMEM(q_shape, jnp.int16),
            pltpu.VMEM((chunks, 2, groups, levels, cw), jnp.int16),
            pltpu.VMEM((groups, 1, LANES), jnp.float32),
            pltpu.VMEM((groups, 1, LANES), jnp.float32),
            pltpu.VMEM((2 * total, cw), jnp.bfloat16),
            pltpu.VMEM((2 * total, cw), jnp.bfloat16),
            pltpu.VMEM((2 * total, cw), jnp.float32),
            pltpu.VMEM(q_shape, jnp.int16),
            pltpu.VMEM(s_shape, jnp.float32),
            pltpu.VMEM(s_shape, jnp.float32),
            dma((3,)), dma((2,)), dma((2,)), dma((2,)),
            dma((chunks,)), dma((chunks,)), dma, dma,
            dma((chunks,)), dma((chunks,)), dma((chunks,)), dma((chunks,)), dma,
        ],
        compiler_params=pltpu.CompilerParams(
            collective_id=0, has_side_effects=True, vmem_limit_bytes=56 * 2**20),
        name="radial_step",
    )(weights, nonlin, state, inverse, pair_of_slot)

    parts = 8
    return pl.pallas_call(
        functools.partial(decode_kernel, parts, groups, width),
        out_shape=jax.ShapeDtypeStruct(state.shape, jnp.float32),
        in_specs=[anywhere] * 2,
        out_specs=anywhere,
        scratch_shapes=[
            pltpu.VMEM(q_shape, jnp.int16),
            pltpu.VMEM(s_shape, jnp.float32),
            pltpu.VMEM(state.shape, jnp.float32),
            dma, dma((parts,)), dma((parts,)),
        ],
        name="decode",
    )(outq, outs)


def solution(mesh):
    placed = (
        P(None, "rad", "ang"),
        P(None, "rad", "ang"),
        P(("ang", "rad"), None, None, None),
        P(("ang", "rad")),
    )
    return jax.shard_map(
        local, mesh=mesh, in_specs=placed, out_specs=P(None, "rad", "ang"), check_vma=False
    )
```
